8 devices in a mesh: stage: 2 (over z, y), expert: 4 (over x, core).
Axes of the slice: x: 2, y: 2, z: 1, core: 2. Of those that a mesh axis runs over, the one named last changes fastest.
Arguments:
- x_act: bfloat16 [2, 8192, 2048], P('stage', 'expert')
- route_idx: int32 [2, 8192, 2], P('stage', 'expert')
- route_wts: float32 [2, 8192, 2], P('stage', 'expert')
- w_one: bfloat16 [2, 8, 2048, 768], P('stage', 'expert')
- w_three: bfloat16 [2, 8, 2048, 768], P('stage', 'expert')
- w_two: bfloat16 [2, 8, 768, 2048], P('stage', 'expert')
- dy_act: bfloat16 [2, 8192, 2048], P('stage', 'expert')
Outputs:
- output 1: bfloat16 [2, 8192, 2048], P('stage', 'expert')
- output 2: bfloat16 [2, 8192, 2048], P('stage', 'expert')
- output 3: bfloat16 [2, 8, 2048, 768], P('stage', 'expert')
- output 4: bfloat16 [2, 8, 2048, 768], P('stage', 'expert')
- output 5: bfloat16 [2, 8, 768, 2048], P('stage', 'expert')
All inputs are finite; a program needn't handle non-finite values.
Results may differ from the reference program's by a relative error of at most 0.0123829.
Values are sent between devices in bfloat16 or wider.
A program may use at most 1 GiB of HBM per device.

```python
import jax
import jax.numpy as jnp
from jax import lax

STAGES = 2
EXPERT_DEVS = 4
TOK_DEV = 2048
MODEL_DIM = 2048
FFN_DIM = 768
EXPERTS = 8
TOP_K = 2
ROUTE_DEVS = 2

LOCAL_EXP = EXPERTS // EXPERT_DEVS
CAPACITY = 2 * TOK_DEV * TOP_K // EXPERTS - 1
TOKENS = EXPERT_DEVS * TOK_DEV
N_SLOT = TOK_DEV * TOP_K


def draw_routing(rng_key):
    n_blocks = EXPERTS // TOP_K
    mean_load = TOK_DEV * TOP_K // EXPERTS
    group_devs = min(ROUTE_DEVS, EXPERT_DEVS)
    group_exp = group_devs * LOCAL_EXP
    key_pair, key_shift, key_tok, key_grp, key_dev = jax.random.split(rng_key, 5)
    block_ids = jnp.broadcast_to(jnp.arange(n_blocks, dtype=jnp.int32), (STAGES, n_blocks))
    pair_perm = jax.random.permutation(key_pair, block_ids, axis=1, independent=True)
    shifts = jax.random.randint(key_shift, (STAGES, EXPERT_DEVS, n_blocks // 2), 0, mean_load)
    shifts = shifts.at[:, :, 0].set(mean_load - 1)
    pair_sign = jnp.array([1, -1], dtype=jnp.int32)
    delta_pos = (shifts[:, :, :, None] * pair_sign).reshape(STAGES, EXPERT_DEVS, n_blocks)
    inv_perm = jnp.broadcast_to(jnp.argsort(pair_perm, axis=1)[:, None, :], delta_pos.shape)
    blk_load = mean_load + jnp.take_along_axis(delta_pos, inv_perm, axis=2)
    blk_ends = jnp.cumsum(blk_load, axis=2)
    tok_pos = jnp.arange(TOK_DEV, dtype=jnp.int32)
    blk_of = jnp.sum((blk_ends[:, :, None, :] <= tok_pos[None, None, :, None]).astype(jnp.int32), axis=3)
    blk_of = jax.random.permutation(key_tok, blk_of, axis=2, independent=True)
    virt_ids = blk_of[:, :, :, None] * TOP_K + jnp.arange(TOP_K, dtype=jnp.int32)
    virt_flat = virt_ids.reshape(STAGES, TOKENS * TOP_K)
    inner_ids = jnp.broadcast_to(jnp.arange(group_exp, dtype=jnp.int32), (STAGES, EXPERTS // group_exp, group_exp))
    grp_perm = jax.random.permutation(key_grp, inner_ids, axis=2, independent=True).reshape(STAGES, EXPERTS)
    dev_ids = jnp.broadcast_to(jnp.arange(EXPERT_DEVS, dtype=jnp.int32), (STAGES, EXPERT_DEVS))
    dev_perm = jax.random.permutation(key_dev, dev_ids, axis=1, independent=True)
    in_group = jnp.take_along_axis(grp_perm, virt_flat, axis=1)
    pre_dev = (virt_flat // group_exp) * group_devs + in_group // LOCAL_EXP
    dest_dev = jnp.take_along_axis(dev_perm, pre_dev, axis=1)
    expert_id = dest_dev * LOCAL_EXP + in_group % LOCAL_EXP
    return expert_id.reshape(STAGES, TOKENS, TOP_K)


def setup_inputs(seed: int = 0) -> dict:
    rng_key = jax.random.key(seed)
    key_x, key_idx, key_wts, key_one, key_three, key_two, key_dy = jax.random.split(rng_key, 7)
    x_act = jax.random.normal(key_x, (STAGES, TOKENS, MODEL_DIM), jnp.float32)
    route_idx = draw_routing(key_idx)
    route_wts = jax.random.uniform(key_wts, (STAGES, TOKENS, TOP_K), jnp.float32, 0.5, 1.5)
    w_one = jax.random.normal(key_one, (STAGES, EXPERTS, MODEL_DIM, FFN_DIM), jnp.float32) * MODEL_DIM ** -0.5
    w_three = jax.random.normal(key_three, (STAGES, EXPERTS, MODEL_DIM, FFN_DIM), jnp.float32) * MODEL_DIM ** -0.5
    w_two = jax.random.normal(key_two, (STAGES, EXPERTS, FFN_DIM, MODEL_DIM), jnp.float32) * FFN_DIM ** -0.5
    dy_act = jax.random.normal(key_dy, (STAGES, TOKENS, MODEL_DIM), jnp.float32)
    return {
        'x_act': x_act.astype(jnp.bfloat16),
        'route_idx': route_idx,
        'route_wts': route_wts,
        'w_one': w_one.astype(jnp.bfloat16),
        'w_three': w_three.astype(jnp.bfloat16),
        'w_two': w_two.astype(jnp.bfloat16),
        'dy_act': dy_act.astype(jnp.bfloat16),
    }


def take_rows(row_table, row_ids):
    return jnp.take(row_table, row_ids, axis=0, mode='fill', fill_value=0)


def stage_tables(idx_blk):
    slot_ids = idx_blk.reshape(N_SLOT)
    hit_mat = (slot_ids[:, None] == jnp.arange(EXPERTS, dtype=jnp.int32)[None, :]).astype(jnp.int32)
    slot_rank = jnp.sum(jnp.cumsum(hit_mat, axis=0) * hit_mat, axis=1) - 1
    buf_pos = slot_ids * CAPACITY + slot_rank
    slot_at = jnp.full((EXPERTS * CAPACITY,), N_SLOT, jnp.int32).at[buf_pos].set(jnp.arange(N_SLOT, dtype=jnp.int32))
    return buf_pos, slot_at


def one_expert(operands):
    x_rows, d_rows, w_in_one, w_in_three, w_out = operands
    pre_one = jnp.dot(x_rows, w_in_one, preferred_element_type=jnp.float32)
    pre_three = jnp.dot(x_rows, w_in_three, preferred_element_type=jnp.float32)
    sig_one = jax.nn.sigmoid(pre_one)
    act_one = pre_one * sig_one
    hidden = (act_one * pre_three).astype(jnp.bfloat16)
    out_rows = jnp.dot(hidden, w_out, preferred_element_type=jnp.float32).astype(jnp.bfloat16)
    d_hidden = jnp.dot(d_rows, w_out.T, preferred_element_type=jnp.float32).astype(jnp.bfloat16).astype(jnp.float32)
    d_three = (d_hidden * act_one).astype(jnp.bfloat16)
    d_one = (d_hidden * pre_three * sig_one * (1.0 + pre_one * (1.0 - sig_one))).astype(jnp.bfloat16)
    dx_rows = (jnp.dot(d_one, w_in_one.T, preferred_element_type=jnp.float32) + jnp.dot(d_three, w_in_three.T, preferred_element_type=jnp.float32)).astype(jnp.bfloat16)
    g_one = jnp.dot(x_rows.T, d_one, preferred_element_type=jnp.float32).astype(jnp.bfloat16)
    g_three = jnp.dot(x_rows.T, d_three, preferred_element_type=jnp.float32).astype(jnp.bfloat16)
    g_two = jnp.dot(hidden.T, d_rows, preferred_element_type=jnp.float32).astype(jnp.bfloat16)
    return out_rows, dx_rows, g_one, g_three, g_two


def to_experts(rows):
    return jnp.transpose(rows.reshape(EXPERT_DEVS, EXPERTS, CAPACITY, MODEL_DIM), (1, 0, 2, 3)).reshape(EXPERTS, EXPERT_DEVS * CAPACITY, MODEL_DIM)


def from_experts(rows):
    return jnp.transpose(rows.reshape(EXPERTS, EXPERT_DEVS, CAPACITY, MODEL_DIM), (1, 0, 2, 3)).reshape(EXPERT_DEVS, EXPERTS * CAPACITY, MODEL_DIM)


def stage_layer(operands):
    x_in, idx_in, wts_in, w_one, w_three, w_two, dy_in = operands
    buf_pos, slot_at = lax.map(stage_tables, idx_in.reshape(EXPERT_DEVS, TOK_DEV, TOP_K))
    x_dev = x_in.reshape(EXPERT_DEVS, TOK_DEV, MODEL_DIM)
    wts_dev = wts_in.reshape(EXPERT_DEVS, TOK_DEV, TOP_K)
    dy_dev = dy_in.reshape(EXPERT_DEVS, TOK_DEV, 1, MODEL_DIM)
    d_slot = (wts_dev[:, :, :, None] * dy_dev.astype(jnp.float32)).astype(jnp.bfloat16).reshape(EXPERT_DEVS, N_SLOT, MODEL_DIM)
    x_exp = to_experts(jax.vmap(take_rows)(x_dev, slot_at // TOP_K))
    d_exp = to_experts(jax.vmap(take_rows)(d_slot, slot_at))
    out_exp, dx_exp, dw_one, dw_three, dw_two = lax.map(one_expert, (x_exp, d_exp, w_one, w_three, w_two))
    out_slot = jax.vmap(take_rows)(from_experts(out_exp), buf_pos).reshape(EXPERT_DEVS, TOK_DEV, TOP_K, MODEL_DIM)
    dx_slot = jax.vmap(take_rows)(from_experts(dx_exp), buf_pos).reshape(EXPERT_DEVS, TOK_DEV, TOP_K, MODEL_DIM)
    y_out = jnp.sum(wts_dev[:, :, :, None] * out_slot.astype(jnp.float32), axis=2).astype(jnp.bfloat16)
    dx_out = jnp.sum(dx_slot.astype(jnp.float32), axis=2).astype(jnp.bfloat16)
    return y_out.reshape(TOKENS, MODEL_DIM), dx_out.reshape(TOKENS, MODEL_DIM), dw_one, dw_three, dw_two


def reference(x_act, route_idx, route_wts, w_one, w_three, w_two, dy_act):
    x_in = jnp.roll(x_act, 1, axis=0)
    idx_in = jnp.roll(route_idx, 1, axis=0)
    wts_in = jnp.roll(route_wts, 1, axis=0)
    y_act, dx_dst, dw_one, dw_three, dw_two = lax.map(stage_layer, (x_in, idx_in, wts_in, w_one, w_three, w_two, dy_act))
    dx_act = jnp.roll(dx_dst, -1, axis=0)
    return (y_act, dx_act, dw_one, dw_three, dw_two)
```

```python
import functools

import jax
import jax.numpy as jnp
from jax import lax
from jax.experimental import pallas as pl
from jax.experimental.pallas import tpu as pltpu
from jax.sharding import PartitionSpec as P


TILE = 256
LANES = 128
VMEM_BYTES = 60 * 1024 * 1024
NT = (((1,), (1,)), ((), ()))
TN = (((0,), (0,)), ((), ()))


def dot(lhs, rhs):
    return jnp.dot(lhs, rhs, preferred_element_type=jnp.float32)


def dot_nt(lhs, rhs):
    return lax.dot_general(lhs, rhs, NT, preferred_element_type=jnp.float32)


def dot_tn(lhs, rhs):
    return lax.dot_general(lhs, rhs, TN, preferred_element_type=jnp.float32)


def gate_cols(gates, pos):
    lane = lax.broadcasted_iota(jnp.int32, gates.shape, 1)
    g_cur = jnp.sum(jnp.where(lane == pos, gates, 0.0), axis=1, keepdims=True)
    g_prev = jnp.sum(jnp.where(lane < pos, gates, 0.0), axis=1, keepdims=True)
    return g_cur, g_prev


def weight_stream(groups, bufs, sems):
    n_local = groups[0][0].shape[0]

    def start(pos, slot):
        for grp in range(len(groups)):
            @pl.when(pos // n_local == grp)
            def _():
                for mat in range(3):
                    pltpu.make_async_copy(groups[grp][mat].at[pos % n_local], bufs[mat].at[slot], sems.at[slot, mat]).start()

    def wait(slot):
        for mat in range(3):
            pltpu.make_async_copy(groups[0][mat].at[0], bufs[mat].at[slot], sems.at[slot, mat]).wait()

    return start, wait


def fwd_kernel(n_grp, act_ref, gate_ref, x_ref, *refs):
    w_refs, (y_ref, b_one, b_three, b_two, sems) = refs[:3 * n_grp], refs[3 * n_grp:]
    groups = [w_refs[3 * k:3 * k + 3] for k in range(n_grp)]
    n_pos = n_grp * groups[0][0].shape[0]
    n_tile = x_ref.shape[0] // TILE
    start, wait = weight_stream(groups, (b_one, b_three, b_two), sems)
    start(0, 0)
    y_ref[...] = jnp.zeros_like(y_ref)

    def expert(pos, _):
        slot = lax.rem(pos, 2)
        wait(slot)

        @pl.when(pos + 1 < n_pos)
        def _():
            start(pos + 1, 1 - slot)

        def tile(m, _):
            @pl.when(act_ref[pos * n_tile + m] > 0)
            def _():
                rows = pl.ds(pl.multiple_of(m * TILE, TILE), TILE)
                x = x_ref[rows, :]
                pre_one = dot(x, b_one[slot])
                pre_three = dot(x, b_three[slot])
                hidden = (pre_one * jax.nn.sigmoid(pre_one) * pre_three).astype(jnp.bfloat16)
                out = dot(hidden, b_two[slot]).astype(jnp.bfloat16)
                g_cur, g_prev = gate_cols(gate_ref[rows, :], pos)
                acc = y_ref[rows, :]
                both = (g_prev * acc.astype(jnp.float32) + g_cur * out.astype(jnp.float32)).astype(jnp.bfloat16)
                y_ref[rows, :] = jnp.where(g_cur > 0, jnp.where(g_prev > 0, both, out), acc)
            return 0

        return lax.fori_loop(0, n_tile, tile, 0)

    lax.fori_loop(0, n_pos, expert, 0)


def hidden_grads(x, d_out, w_in_one, w_in_three, w_out):
    pre_one = dot(x, w_in_one)
    pre_three = dot(x, w_in_three)
    d_hidden = dot_nt(d_out, w_out).astype(jnp.bfloat16).astype(jnp.float32)
    sig_one = jax.nn.sigmoid(pre_one)
    act_one = pre_one * sig_one
    d_three = d_hidden * act_one
    d_one = d_hidden * pre_three * sig_one * (1.0 + pre_one * (1.0 - sig_one))
    return act_one * pre_three, d_one, d_three


def dx_kernel(n_grp, act_ref, gate_ref, x_ref, dy_ref, *refs):
    w_refs, (dx_ref, b_one, b_three, b_two, sems) = refs[:3 * n_grp], refs[3 * n_grp:]
    groups = [w_refs[3 * k:3 * k + 3] for k in range(n_grp)]
    n_pos = n_grp * groups[0][0].shape[0]
    n_tile = x_ref.shape[0] // TILE
    start, wait = weight_stream(groups, (b_one, b_three, b_two), sems)
    start(0, 0)
    dx_ref[...] = jnp.zeros_like(dx_ref)

    def expert(pos, _):
        slot = lax.rem(pos, 2)
        wait(slot)

        @pl.when(pos + 1 < n_pos)
        def _():
            start(pos + 1, 1 - slot)

        def tile(m, _):
            @pl.when(act_ref[pos * n_tile + m] > 0)
            def _():
                rows = pl.ds(pl.multiple_of(m * TILE, TILE), TILE)
                g_cur, g_prev = gate_cols(gate_ref[rows, :], pos)
                d_out = (g_cur * dy_ref[rows, :].astype(jnp.float32)).astype(jnp.bfloat16)
                _, d_one, d_three = hidden_grads(x_ref[rows, :], d_out, b_one[slot], b_three[slot], b_two[slot])
                dx = (dot_nt(d_one.astype(jnp.bfloat16), b_one[slot]) + dot_nt(d_three.astype(jnp.bfloat16), b_three[slot])).astype(jnp.bfloat16)
                acc = dx_ref[rows, :]
                both = (acc.astype(jnp.float32) + dx.astype(jnp.float32)).astype(jnp.bfloat16)
                dx_ref[rows, :] = jnp.where(g_cur > 0, jnp.where(g_prev > 0, both, dx), acc)
            return 0

        return lax.fori_loop(0, n_tile, tile, 0)

    lax.fori_loop(0, n_pos, expert, 0)


def dw_kernel(n_src, has_acc, last, cnt_ref, list_ref, gate_ref, *refs):
    refs = list(refs)
    x_refs = [refs.pop(0) for _ in range(n_src)]
    dy_refs = [refs.pop(0) for _ in range(n_src)]
    w_one, w_three, w_two = [refs.pop(0) for _ in range(3)]
    acc_in = [refs.pop(0) for _ in range(3)] if has_acc else None
    outs = [refs.pop(0) for _ in range(3)]
    acc = [refs.pop(0) for _ in range(3)]
    x_buf, dy_buf, t_sems, a_sems = refs[:4]
    stage_bufs = refs[4:]
    q = pl.program_id(0)
    n_tile = gate_ref.shape[0] // TILE
    n_act = cnt_ref[q]

    def start(step, slot):
        tid = list_ref[q, step]
        row = pl.ds(pl.multiple_of(lax.rem(tid, n_tile) * TILE, TILE), TILE)
        for k in range(n_src):
            @pl.when(tid // n_tile == k)
            def _():
                pltpu.make_async_copy(x_refs[k].at[row, :], x_buf.at[slot], t_sems.at[slot, 0]).start()
                pltpu.make_async_copy(dy_refs[k].at[row, :], dy_buf.at[slot], t_sems.at[slot, 1]).start()

    @pl.when(n_act > 0)
    def _():
        start(0, 0)

    if has_acc:
        copies = [pltpu.make_async_copy(acc_in[mat].at[q], acc[mat], a_sems.at[mat]) for mat in range(3)]
        for copy in copies:
            copy.start()
        for copy in copies:
            copy.wait()
    else:
        for mat in range(3):
            acc[mat][...] = jnp.zeros_like(acc[mat])

    def body(step, _):
        slot = lax.rem(step, 2)
        tid = list_ref[q, step]
        pltpu.make_async_copy(x_refs[0].at[pl.ds(0, TILE), :], x_buf.at[slot], t_sems.at[slot, 0]).wait()
        pltpu.make_async_copy(dy_refs[0].at[pl.ds(0, TILE), :], dy_buf.at[slot], t_sems.at[slot, 1]).wait()

        @pl.when(step + 1 < n_act)
        def _():
            start(step + 1, 1 - slot)

        gates = gate_ref[pl.ds(pl.multiple_of(lax.rem(tid, n_tile) * TILE, TILE), TILE), :]
        g_cur, _ = gate_cols(gates, (tid // n_tile) * 2 + q)
        chosen = g_cur > 0
        x = x_buf[slot]
        d_out = (g_cur * dy_buf[slot].astype(jnp.float32)).astype(jnp.bfloat16)
        hidden, d_one, d_three = hidden_grads(x, d_out, w_one[0], w_three[0], w_two[0])
        hidden = jnp.where(chosen, hidden, 0.0).astype(jnp.bfloat16)
        d_one = jnp.where(chosen, d_one, 0.0).astype(jnp.bfloat16)
        d_three = jnp.where(chosen, d_three, 0.0).astype(jnp.bfloat16)
        acc[0][...] += dot_tn(x, d_one)
        acc[1][...] += dot_tn(x, d_three)
        acc[2][...] += dot_tn(hidden, d_out)
        return 0

    lax.fori_loop(0, n_act, body, 0)

    copies = []
    for mat in range(3):
        src = acc[mat]
        if last:
            src = stage_bufs[mat]
            src[...] = acc[mat][...].astype(jnp.bfloat16)
        copies.append(pltpu.make_async_copy(src, outs[mat].at[q], a_sems.at[mat]))
        copies[-1].start()
    for copy in copies:
        copy.wait()


ANY = pl.BlockSpec(memory_space=pl.ANY)
SMEM = pl.BlockSpec(memory_space=pltpu.SMEM)
VMEM = pl.BlockSpec(memory_space=pltpu.VMEM)


def params():
    return pltpu.CompilerParams(vmem_limit_bytes=VMEM_BYTES)


def weight_bufs(w_one, w_two):
    return [
        pltpu.VMEM((2,) + w_one.shape[1:], jnp.bfloat16),
        pltpu.VMEM((2,) + w_one.shape[1:], jnp.bfloat16),
        pltpu.VMEM((2,) + w_two.shape[1:], jnp.bfloat16),
        pltpu.SemaphoreType.DMA((2, 3)),
    ]


def run_fwd(act, gates, x, groups):
    n_tok, d = x.shape
    f = groups[0][0].shape[2]
    w_flat = [m for g in groups for m in g]
    return pl.pallas_call(
        functools.partial(fwd_kernel, len(groups)),
        out_shape=jax.ShapeDtypeStruct((n_tok, d), jnp.bfloat16),
        in_specs=[SMEM, VMEM, VMEM] + [ANY] * len(w_flat),
        out_specs=VMEM,
        scratch_shapes=weight_bufs(groups[0][0], groups[0][2]),
        compiler_params=params(),
        cost_estimate=pl.CostEstimate(flops=2 * 3 * 2 * n_tok * d * f, bytes_accessed=100_000_000, transcendentals=0),
        name="fwd_tiles",
    )(act, gates, x, *w_flat)


def run_dx(act, gates, x, dy, groups):
    n_tok, d = x.shape
    f = groups[0][0].shape[2]
    w_flat = [m for g in groups for m in g]
    return pl.pallas_call(
        functools.partial(dx_kernel, len(groups)),
        out_shape=jax.ShapeDtypeStruct((n_tok, d), jnp.bfloat16),
        in_specs=[SMEM, VMEM, VMEM, VMEM] + [ANY] * len(w_flat),
        out_specs=VMEM,
        scratch_shapes=weight_bufs(groups[0][0], groups[0][2]),
        compiler_params=params(),
        cost_estimate=pl.CostEstimate(flops=2 * 5 * 2 * n_tok * d * f, bytes_accessed=100_000_000, transcendentals=0),
        name="dx_tiles",
    )(act, gates, x, dy, *w_flat)


def run_dw(cnt, tiles, gates, xs, dys, weights, acc, last):
    d, f = weights[0].shape[1:]
    n_src = len(xs)
    n_local = weights[0].shape[0]
    shapes = [(d, f), (d, f), (f, d)]
    out_dtype = jnp.bfloat16 if last else jnp.float32
    w_specs = [pl.BlockSpec((1,) + s, lambda q: (q, 0, 0)) for s in shapes]
    return pl.pallas_call(
        functools.partial(dw_kernel, n_src, acc is not None, last),
        grid=(n_local,),
        out_shape=[jax.ShapeDtypeStruct((n_local,) + s, out_dtype) for s in shapes],
        in_specs=[SMEM, SMEM, pl.BlockSpec(gates.shape, lambda q: (0, 0))] + [ANY] * (2 * n_src) + w_specs + [ANY] * (3 if acc is not None else 0),
        out_specs=[ANY] * 3,
        scratch_shapes=[pltpu.VMEM(s, jnp.float32) for s in shapes] + [
            pltpu.VMEM((2, TILE, d), jnp.bfloat16),
            pltpu.VMEM((2, TILE, d), jnp.bfloat16),
            pltpu.SemaphoreType.DMA((2, 2)),
            pltpu.SemaphoreType.DMA((3,)),
        ] + ([pltpu.VMEM(s, jnp.bfloat16) for s in shapes] if last else []),
        compiler_params=params(),
        cost_estimate=pl.CostEstimate(flops=2 * 6 * n_src * xs[0].shape[0] * d * f, bytes_accessed=100_000_000, transcendentals=0),
        name="dw_tiles",
    )(cnt, tiles, gates, *xs, *dys, *weights, *(acc or ()))


def sort_rows(rank, rows):
    n = rank.shape[0]
    pick = (lax.broadcasted_iota(jnp.int32, (n, n), 0) == rank[None, :]).astype(jnp.bfloat16)
    return jnp.dot(pick, rows, preferred_element_type=jnp.float32).astype(jnp.bfloat16)


def unsort_rows(rank, rows):
    n = rank.shape[0]
    pick = (lax.broadcasted_iota(jnp.int32, (n, n), 1) == rank[:, None]).astype(jnp.bfloat16)
    return jnp.dot(pick, rows, preferred_element_type=jnp.float32).astype(jnp.bfloat16)


def solution(mesh):
    n_stage = mesh.shape['stage']
    n_dev = mesh.shape['expert']
    to_next = [(k, (k + 1) % n_stage) for k in range(n_stage)]
    to_prev = [((k + 1) % n_stage, k) for k in range(n_stage)]
    cross = [(k, k ^ 2) for k in range(n_dev)]
    core = [(k, k ^ 1) for k in range(n_dev)]
    tok_spec = P('stage', 'expert', None)
    w_spec = P('stage', 'expert', None, None)

    def moe_layer(x_act, route_idx, route_wts, w_one, w_three, w_two, dy_act):
        x_src = x_act[0]
        n_tok, d = x_src.shape
        n_local = w_one.shape[1]
        n_exp = n_local * n_dev
        n_tile = n_tok // TILE
        me = lax.axis_index('expert')

        w_own = (w_one[0], w_three[0], w_two[0])
        w_x = tuple(lax.ppermute(w, 'expert', cross) for w in w_own)
        w_c = tuple(lax.ppermute(w, 'expert', core) for w in w_own)
        w_d = tuple(lax.ppermute(w, 'expert', core) for w in w_x)

        idx = route_idx[0]
        lo, hi = jnp.min(idx, axis=1), jnp.max(idx, axis=1)
        tok_ids = jnp.arange(n_tok, dtype=jnp.int32)
        key = (lo * n_exp + hi) * n_tok + tok_ids
        rank = jnp.sum((key[None, :] < key[:, None]).astype(jnp.int32), axis=1)
        hit = lax.broadcasted_iota(jnp.int32, (n_tok, n_tok), 0) == rank[None, :]
        cols = [idx[:, 0].astype(jnp.float32), idx[:, 1].astype(jnp.float32), route_wts[0][:, 0], route_wts[0][:, 1]]
        meta = [jnp.sum(jnp.where(hit, c[None, :], 0.0), axis=1) for c in cols] + [rank.astype(jnp.float32)]
        meta = jnp.stack(meta + [jnp.zeros_like(meta[0])] * 3)
        meta = lax.ppermute(meta, 'stage', to_next)
        metas = lax.all_gather(meta, 'expert')
        rank_own = meta[4].astype(jnp.int32)

        xs = sort_rows(rank, x_src)
        x_fwd = lax.ppermute(xs, 'stage', to_next)
        xs_again, _ = lax.optimization_barrier((xs, meta))
        x_bwd = lax.ppermute(xs_again, 'stage', to_next)

        dys = sort_rows(rank_own, dy_act[0])
        dy_c = lax.ppermute(dys, 'expert', core)
        dy_x = lax.ppermute(dys, 'expert', cross)
        dy_d = lax.ppermute(dy_x, 'expert', core)
        x_c = lax.ppermute(x_bwd, 'expert', core)
        x_x = lax.ppermute(x_bwd, 'expert', cross)
        x_d = lax.ppermute(x_x, 'expert', core)

        def gates_of(tab, expert_ids):
            e_first, e_second = tab[0].astype(jnp.int32)[:, None], tab[1].astype(jnp.int32)[:, None]
            return jnp.where(e_first == expert_ids, tab[2][:, None], 0.0) + jnp.where(e_second == expert_ids, tab[3][:, None], 0.0)

        lane = jnp.arange(LANES, dtype=jnp.int32)
        pos_exp = jnp.where(lane < n_exp, n_local * jnp.bitwise_xor(me, lane // n_local) + lane % n_local, -1)[None, :]
        gates = gates_of(meta, pos_exp)
        act = (jnp.max(gates[:, :n_exp].reshape(n_tile, TILE, n_exp), axis=1) > 0).astype(jnp.int32).T.reshape(-1)

        src_order = [jnp.bitwise_xor(me, k) for k in range(n_dev)]
        own_exp = n_local * me + jnp.arange(n_local, dtype=jnp.int32)[None, :]
        gates_all = jnp.concatenate([gates_of(lax.dynamic_index_in_dim(metas, s, 0, False), own_exp) for s in src_order], axis=1)

        def tile_list(g):
            hits = (jnp.max(g.reshape(n_tile, TILE, -1, n_local), axis=1) > 0).astype(jnp.int32)
            hits = jnp.transpose(hits, (2, 1, 0)).reshape(n_local, -1)
            place = jnp.cumsum(hits, axis=1) - 1
            n = hits.shape[1]
            ids = jnp.arange(n, dtype=jnp.int32)
            sel = (place[:, None, :] == ids[None, :, None]) & (hits[:, None, :] > 0)
            return jnp.sum(hits, axis=1), jnp.sum(jnp.where(sel, ids[None, None, :], 0), axis=2)

        def pad_lanes(g):
            return jnp.pad(g, ((0, 0), (0, LANES - g.shape[1])))

        near, far = gates_all[:, :2 * n_local], gates_all[:, 2 * n_local:]
        cnt_near, list_near = tile_list(near)
        cnt_far, list_far = tile_list(far)

        groups = (w_own, w_c, w_x, w_d)
        acc = run_dw(cnt_near, list_near, pad_lanes(near), (x_bwd, x_c), (dys, dy_c), w_own, None, False)
        dxs = run_dx(act, gates, x_bwd, dys, groups)
        dx_back = lax.ppermute(dxs, 'stage', to_prev)
        ys = run_fwd(act, gates, x_fwd, groups)
        y_own = unsort_rows(rank_own, ys)
        g_one, g_three, g_two = run_dw(cnt_far, list_far, pad_lanes(far), (x_x, x_d), (dy_x, dy_d), w_own, tuple(acc), True)
        dx_own = unsort_rows(rank, dx_back)
        return y_own[None], dx_own[None], g_one[None], g_three[None], g_two[None]

    return jax.shard_map(moe_layer, mesh=mesh, in_specs=(tok_spec, tok_spec, tok_spec, w_spec, w_spec, w_spec, tok_spec), out_specs=(tok_spec, tok_spec, w_spec, w_spec, w_spec), check_vma=False)
```
